32 devices in a mesh: seq: 4 (over y, x), batch: 8 (over z, core).
Axes of the slice: x: 2, y: 2, z: 4, core: 2. Of those that a mesh axis runs over, the one named last changes fastest.
Arguments:
- attn_out: bfloat16 [16384, 2560], P(('seq', 'batch')), may hold values from -200 to 200
- out_grad: bfloat16 [16384, 2560], P(('seq', 'batch')), may hold values from -6 to 6
- master: float32 [2560, 2560], P(('seq', 'batch')), may hold values from -0.125 to 0.125
- moment_one: float32 [2560, 2560], P(('seq', 'batch')), may hold values from -4 to 4
- moment_two: float32 [2560, 2560], P(('seq', 'batch')), may hold values from 0.002 to 0.05
Outputs:
- input_grad: bfloat16 [16384, 2560], P(('seq', 'batch'))
- new_master: float32 [2560, 2560], P(('seq', 'batch'))
- new_moment_one: float32 [2560, 2560], P(('seq', 'batch'))
- new_moment_two: float32 [2560, 2560], P(('seq', 'batch'))
The draws below stay inside these ranges and needn't reach their ends.
All inputs are finite; a program needn't handle non-finite values.
Results may differ from the reference program's by a relative error of at most 0.01.
Values may be sent and summed in bfloat16 or wider, within the bound.
A program may use at most 128 MiB of HBM per device.

```python
import math
import jax
import jax.numpy as jnp
from jax import lax

DIN = 2560
DOUT = 2560
TOK_DEV = 512
STEP = 10
TOKENS = 16384


def draw_attn_out(key, part):
    blocks = TOKENS // TOK_DEV
    feature_width = DIN // blocks
    first_key, second_key = jax.random.split(jax.random.fold_in(key, 11), 2)
    ramp = jnp.arange(DIN, dtype=jnp.float32) / jnp.float32(DIN)
    values = jax.random.normal(first_key, (TOKENS, DIN), jnp.float32)
    column = 10.0 ** ramp
    pairing = jax.random.permutation(second_key, blocks)
    token_block = jnp.arange(TOKENS) // TOK_DEV
    feature_block = jnp.arange(DIN) // feature_width
    spike = jnp.where(pairing[token_block][:, None] == feature_block[None, :], 6.0, 1.0)
    result = jnp.clip(values * column[None, :] * spike, -200.0, 200.0)
    return result.astype(jnp.bfloat16)


def steps_of(rng, shape, pieces, least, largest):
    factor_of, own = 1.0, jax.random.fold_in(rng, 6)
    for dim, parts in pieces:
        heights = jnp.exp(jax.random.uniform(jax.random.fold_in(own, dim), (parts,), jnp.float32, least / len(pieces), largest / len(pieces)))
        factor_of = factor_of * jnp.repeat(heights, shape[dim] // parts).reshape([-1 if axis == dim else 1 for axis in range(len(shape))])
    return factor_of


def noise(stream_key, extent, spread, most, shards=(), kind=jnp.bfloat16):
    drawn = jax.random.normal(stream_key, extent, jnp.float32) * spread
    if len(shards) > 0:
        drawn = steps_of(stream_key, extent, shards, -0.22, 0.18) * drawn
    return jnp.clip(drawn, min=-most, max=most).astype(kind)


def setup_inputs(seed: int = 0) -> dict:
    key_list = jax.random.split(jax.random.key(seed), 6)
    attn_out = draw_attn_out(jax.random.fold_in(key_list[5], 71), 0)
    out_grad = noise(key_list[1], (TOKENS, DOUT), 1.0, 6.0, ((0, 32),))
    master = noise(key_list[2], (DIN, DOUT), DIN ** -0.5, 0.125, ((0, 32),), jnp.float32)
    moment_one = noise(key_list[3], (DIN, DOUT), 0.3, 4.0, ((0, 32),), jnp.float32)
    moment_two = jnp.clip(jnp.exp(math.log(0.05) - 3.218876 * jax.random.uniform(key_list[4], (DIN, DOUT), jnp.float32) ** steps_of(key_list[4], (DIN, DOUT), ((0, 32),), -0.2, 0.2)), 0.002, 0.05)
    return dict(attn_out=attn_out, out_grad=out_grad, master=master, moment_one=moment_one, moment_two=moment_two)


def reference(attn_out, out_grad, master, moment_one, moment_two):
    weight = master.astype(jnp.bfloat16)
    input_grad = lax.dot_general(out_grad, weight, (((1,), (1,)), ((), ())), preferred_element_type=jnp.float32).astype(jnp.bfloat16)
    weight_grad = lax.dot_general(attn_out, out_grad, (((0,), (0,)), ((), ())), preferred_element_type=jnp.float32)
    grad_norm = jnp.sqrt(jnp.sum(weight_grad * weight_grad)) + 1e-06
    limit = jnp.sqrt(jnp.float32(DIN * DOUT))
    clipped = weight_grad * jnp.minimum(jnp.float32(1.0), limit / grad_norm)
    new_one = 0.9 * moment_one + 0.1 * clipped
    new_two = 0.999 * moment_two + 0.001 * clipped * clipped
    first_hat = new_one / (1.0 - 0.9 ** STEP)
    second_hat = new_two / (1.0 - 0.999 ** STEP)
    new_master = master - 0.01 * (first_hat / (jnp.sqrt(second_hat) + 1e-08) + 0.1 * master)
    return (input_grad, new_master, new_one, new_two)
```

```python
import functools
import jax
import jax.numpy as jnp
from jax import lax
from jax.experimental import pallas as pl
from jax.experimental.pallas import tpu as pltpu
from jax.sharding import PartitionSpec as P

GRAD_BLOCKS = 4
STEP = 10
MESH = pl.DeviceIdType.MESH
F32 = jnp.float32
BF16 = jnp.bfloat16


def kernel(nb, attn_ref, og_ref, w_ref, ig_ref, gw_ref, sq_ref,
           rx_attn, rx_og, tbuf, attn_t, wg, g, r1a, r1b, r2, t2, pz, rz, sqs,
           x_s, x_r, z_s, z_r, p_s, p_r, d_s, d_r, c_s, c_r,
           s1_s, s1_r, s2_s, s2_r, rz_s, rz_r, q_s, q_r):
    ns = 4
    nz = nb // 2
    tok, din = attn_ref.shape
    dout = og_ref.shape[1]
    r = w_ref.shape[0]
    half = dout // 2
    block = nb * r
    seq = lax.axis_index("seq")
    batch = lax.axis_index("batch")
    z = batch // 2
    core = batch % 2
    hi = seq // 2
    lo = seq % 2
    sh = (1 - hi) * 2 + lo
    sl = hi * 2 + (1 - lo)
    sd = (1 - hi) * 2 + (1 - lo)
    hi_dev = (sh, batch)
    lo_dev = (sl, batch)
    core_dev = (seq, z * 2 + 1 - core)
    cols_a = pl.ds(0, half)
    cols_b = pl.ds(half, half)

    def other(i):
        f = lax.rem(seq * nb + batch + i, ns * nb)
        return (f // nb, lax.rem(f, nb))

    barrier = pltpu.get_barrier_semaphore()

    def greet(i, carry):
        pl.semaphore_signal(barrier, inc=1, device_id=other(i), device_id_type=MESH)
        return carry

    lax.fori_loop(1, ns * nb, greet, 0)
    pl.semaphore_wait(barrier, ns * nb - 1)

    pending = []

    def remote(src, dst, ssem, rsem, dev):
        c = pltpu.make_async_remote_copy(
            src_ref=src, dst_ref=dst, send_sem=ssem, recv_sem=rsem,
            device_id=dev, device_id_type=MESH)
        c.start()
        pending.append(c)
        return c

    def zk(k):
        return lax.rem(z + nz - k, nz)

    def wrows(s, zz):
        return pl.ds(pl.multiple_of((s * nb + zz * 2 + core) * r, 16), r)

    def shard(k):
        return w_ref if k == 0 else wg.at[wrows(seq, zk(k))]

    own = wrows(seq, z)
    zc, hc, lc, dac, dbc, cc = {}, {}, {}, {}, {}, {}

    def plane_send(k):
        rows = wrows(seq, zk(k))
        hc[k] = remote(shard(k), wg.at[rows], p_s.at[2 * k], p_r.at[2 * k], hi_dev)
        lc[k] = remote(shard(k), wg.at[rows], p_s.at[2 * k + 1], p_r.at[2 * k + 1], lo_dev)

    def core_send(k, j, s):
        rows = wrows(s, zk(k))
        src = w_ref if (k == 0 and j == 0) else wg.at[rows]
        i = 4 * k + j
        cc[i] = remote(src, wg.at[rows], c_s.at[i], c_r.at[i], core_dev)

    def z_arrive(k):
        zc[k].wait_recv()
        plane_send(k)
        core_send(k, 0, seq)

    def plane_arrive(k):
        hc[k].wait_recv()
        v = wg.at[wrows(sh, zk(k)), cols_a]
        dac[k] = remote(v, v, d_s.at[2 * k], d_r.at[2 * k], lo_dev)
        lc[k].wait_recv()
        v = wg.at[wrows(sl, zk(k)), cols_b]
        dbc[k] = remote(v, v, d_s.at[2 * k + 1], d_r.at[2 * k + 1], hi_dev)
        core_send(k, 1, sh)
        core_send(k, 2, sl)

    def diag_arrive(k):
        dac[k].wait_recv()
        dbc[k].wait_recv()
        core_send(k, 3, sd)

    xa = remote(attn_ref, rx_attn, x_s.at[0], x_r.at[0], core_dev)
    plane_send(0)
    for k in range(1, nz):
        dev = (seq, lax.rem(z + k, nz) * 2 + core)
        zc[k] = remote(w_ref, wg.at[own], z_s.at[k], z_r.at[k], dev)
    xo = remote(og_ref, rx_og, x_s.at[1], x_r.at[1], core_dev)
    core_send(0, 0, seq)
    wg[own, :] = w_ref[...]

    def transpose_in(src, koff):
        for s in range(ns):
            tbuf[...] = src[:, s * block:(s + 1) * block].T
            for zz in range(nz):
                part = tbuf[pl.ds(pl.multiple_of((zz * 2 + core) * r, 16), r), :]
                attn_t[pl.ds((s * nz + zz) * r, r), pl.ds(koff, tok)] = part

    tile = 256 if dout % 256 == 0 and din % 256 == 0 else 128
    ntile = dout // tile

    def grad_tiles(first, last):
        def body(i, carry):
            c = pl.ds(pl.multiple_of(i * tile, tile), tile)
            acc = jnp.dot(attn_t[:, :tok], og_ref[:, c], preferred_element_type=F32)
            acc += jnp.dot(attn_t[:, tok:], rx_og[:, c], preferred_element_type=F32)
            g[:, c] = acc.astype(BF16)
            return carry
        lax.fori_loop(first, last, body, 0)

    transpose_in(attn_ref, 0)
    if nz > 1:
        z_arrive(1)
    xa.wait_recv()
    transpose_in(rx_attn, tok)
    plane_arrive(0)
    xo.wait_recv()
    for k in range(1, nz):
        grad_tiles((k - 1) * ntile // (nz - 1), k * ntile // (nz - 1))
        if k + 1 < nz:
            z_arrive(k + 1)
        if k < nz - 1:
            plane_arrive(k)

    def grows(s, i):
        return pl.ds(pl.multiple_of((s * nz + lax.rem(z + 1 + i, nz)) * r, 16), r)

    def rr(i):
        return pl.ds(i * r, r)

    s1, s2 = {}, {}

    def stage1(i):
        s1[i] = [
            remote(g.at[grows(sd, i), cols_a], r1a.at[rr(2 * i + 1)], s1_s.at[4 * i], s1_r.at[4 * i], hi_dev),
            remote(g.at[grows(sd, i), cols_b], r1b.at[rr(2 * i + 1)], s1_s.at[4 * i + 1], s1_r.at[4 * i + 1], lo_dev),
            remote(g.at[grows(sh, i), cols_a], r1a.at[rr(2 * i)], s1_s.at[4 * i + 2], s1_r.at[4 * i + 2], hi_dev),
            remote(g.at[grows(sl, i), cols_b], r1b.at[rr(2 * i)], s1_s.at[4 * i + 3], s1_r.at[4 * i + 3], lo_dev),
        ]

    def stage2(i):
        s1[i][0].wait_recv()
        t2[rr(i), cols_a] = (g[grows(sl, i), cols_a].astype(F32) + r1a[rr(2 * i + 1), :].astype(F32)).astype(BF16)
        ca = remote(t2.at[rr(i), cols_a], r2.at[rr(i), cols_a], s2_s.at[2 * i], s2_r.at[2 * i], lo_dev)
        s1[i][1].wait_recv()
        t2[rr(i), cols_b] = (g[grows(sh, i), cols_b].astype(F32) + r1b[rr(2 * i + 1), :].astype(F32)).astype(BF16)
        cb = remote(t2.at[rr(i), cols_b], r2.at[rr(i), cols_b], s2_s.at[2 * i + 1], s2_r.at[2 * i + 1], hi_dev)
        s2[i] = [ca, cb]

    zsum = {}

    def stage3(i):
        for c in (s1[i][2], s1[i][3], s2[i][0], s2[i][1]):
            c.wait_recv()
        for cols, r1 in ((cols_a, r1a), (cols_b, r1b)):
            v = g[grows(seq, i), cols].astype(F32) + r1[rr(2 * i), :].astype(F32) + r2[rr(i), cols].astype(F32)
            if i == nz - 1:
                gw_ref[:, cols] = v
            else:
                pz[rr(i), cols] = v.astype(BF16)
        if i < nz - 1:
            dev = (seq, lax.rem(z + 1 + i, nz) * 2 + core)
            zsum[i] = remote(pz.at[rr(i)], rz.at[rr(i)], rz_s.at[i], rz_r.at[i], dev)

    stage1(0)
    if nz > 1:
        plane_arrive(nz - 1)
    for k in range(nz):
        diag_arrive(k)
        if k == 0 and nz > 1:
            stage1(1)

    def input_tiles(first, last):
        def body(i, carry):
            c = pl.ds(pl.multiple_of(i * tile, tile), tile)
            v = lax.dot_general(og_ref[...], wg[c, :], (((1,), (1,)), ((), ())), preferred_element_type=F32)
            ig_ref[:, c] = v.astype(BF16)
            return carry
        lax.fori_loop(first, last, body, 0)

    itile = din // tile
    stage2(0)
    for i in range(4 * nz):
        cc[i].wait_recv()
    for i in range(nz):
        input_tiles(i * itile // nz, (i + 1) * itile // nz)
        if i + 2 < nz:
            stage1(i + 2)
        if i + 1 < nz:
            stage2(i + 1)
        stage3(i)
    for i in range(nz - 1):
        zsum[i].wait_recv()
        gw_ref[...] += rz[rr(i), :].astype(F32)

    v = gw_ref[...]
    part = jnp.sum((v * v).reshape(r // 8, 8, dout), axis=0)
    acc = part[:, :128]
    for i in range(1, dout // 128):
        acc += part[:, i * 128:(i + 1) * 128]
    sqs[0] = acc

    def q_copy(i):
        return pltpu.make_async_remote_copy(
            src_ref=sqs.at[0], dst_ref=sqs.at[i], send_sem=q_s.at[i], recv_sem=q_r.at[i],
            device_id=other(i), device_id_type=MESH)

    def q_start(i, carry):
        q_copy(i).start()
        return carry

    def q_wait(i, carry):
        q_copy(i).wait()
        return carry

    lax.fori_loop(1, ns * nb, q_start, 0)
    lax.fori_loop(1, ns * nb, q_wait, 0)
    total = sqs[0]
    for i in range(1, ns * nb):
        total += sqs[i]
    sq_ref[...] = total
    for c in pending:
        c.wait_send()


def fused(attn_out, out_grad, shard_weight, ns, nb):
    tok, din = attn_out.shape
    dout = out_grad.shape[1]
    r = shard_weight.shape[0]
    nz = nb // 2
    n = ns * nb
    dma = lambda k: pltpu.SemaphoreType.DMA((k,))
    vm = pl.BlockSpec(memory_space=pltpu.VMEM)
    pairs = [2, nz, 2 * nz, 2 * nz, 4 * nz, 4 * nz, 2 * nz, nz, n]
    return pl.pallas_call(
        functools.partial(kernel, nb),
        out_shape=(
            jax.ShapeDtypeStruct((tok, din), BF16),
            jax.ShapeDtypeStruct((r, dout), F32),
            jax.ShapeDtypeStruct((8, 128), F32),
        ),
        in_specs=[vm] * 3,
        out_specs=(vm,) * 3,
        scratch_shapes=[
            pltpu.VMEM((tok, din), BF16),
            pltpu.VMEM((tok, dout), BF16),
            pltpu.VMEM((nb * r, tok), BF16),
            pltpu.VMEM((din // 2, 2 * tok), BF16),
            pltpu.VMEM((din, dout), BF16),
            pltpu.VMEM((din // 2, dout), BF16),
            pltpu.VMEM((2 * nz * r, dout // 2), BF16),
            pltpu.VMEM((2 * nz * r, dout // 2), BF16),
            pltpu.VMEM((nz * r, dout), BF16),
            pltpu.VMEM((nz * r, dout), BF16),
            pltpu.VMEM((nz * r, dout), BF16),
            pltpu.VMEM((nz * r, dout), BF16),
            pltpu.VMEM((n, 8, 128), F32),
        ] + [dma(k) for k in pairs for _ in range(2)],
        compiler_params=pltpu.CompilerParams(
            collective_id=0, has_side_effects=True, vmem_limit_bytes=66_000_000),
    )(attn_out, out_grad, shard_weight)


def plain(attn_out, out_grad, shard_weight):
    projected = lax.dot_general(
        out_grad,
        lax.all_gather(shard_weight, ("seq", "batch"), axis=0, tiled=True),
        (((1,), (1,)), ((), ())),
        preferred_element_type=F32,
    )
    width = out_grad.shape[1] // GRAD_BLOCKS
    parts = []
    for b in range(GRAD_BLOCKS):
        d = lax.dot_general(
            attn_out, out_grad[:, b * width:(b + 1) * width],
            (((0,), (0,)), ((), ())), preferred_element_type=F32).astype(BF16)
        d = lax.psum_scatter(d, "seq", scatter_dimension=0, tiled=True)
        parts.append(lax.psum_scatter(d, "batch", scatter_dimension=0, tiled=True).astype(F32))
    weight_grad = jnp.concatenate(parts, axis=1)
    squares = lax.psum(jnp.sum(weight_grad * weight_grad), ("seq", "batch"))
    return projected.astype(BF16), weight_grad, squares


def on_device(ns, nb, attn_out, out_grad, master, moment_one, moment_two):
    shard_weight = master.astype(BF16)
    r, dout = master.shape
    din = attn_out.shape[1]
    if ns == 4 and nb % 2 == 0 and r % 16 == 0 and (nb * r) % 128 == 0 and dout % 256 == 0:
        input_grad, weight_grad, sq = fused(attn_out, out_grad, shard_weight, ns, nb)
        squares = jnp.sum(sq)
    else:
        input_grad, weight_grad, squares = plain(attn_out, out_grad, shard_weight)
    grad_norm = jnp.sqrt(squares) + 1e-06
    limit = jnp.sqrt(jnp.float32(din * dout))
    clipped = weight_grad * jnp.minimum(jnp.float32(1.0), limit / grad_norm)
    new_one = 0.9 * moment_one + 0.1 * clipped
    new_two = 0.999 * moment_two + 0.001 * clipped * clipped
    first_hat = new_one / (1.0 - 0.9**STEP)
    second_hat = new_two / (1.0 - 0.999**STEP)
    new_master = master - 0.01 * (first_hat / (jnp.sqrt(second_hat) + 1e-08) + 0.1 * master)
    return (input_grad, new_master, new_one, new_two)


def solution(mesh):
    spec = P(("seq", "batch"), None)
    return jax.shard_map(
        functools.partial(on_device, mesh.shape["seq"], mesh.shape["batch"]),
        mesh=mesh,
        in_specs=(spec,) * 5,
        out_specs=(spec,) * 4,
        check_vma=False,
    )
```

```python
import functools
import jax
import jax.numpy as jnp
from jax import lax
from jax.experimental import pallas as pl
from jax.experimental.pallas import tpu as pltpu
from jax.sharding import PartitionSpec as P

GRAD_BLOCKS = 4
STEP = 10
MESH = pl.DeviceIdType.MESH
F32 = jnp.float32
BF16 = jnp.bfloat16


def kernel(nb, attn_hbm, og_hbm, w_ref, ig_ref, gw_ref, sq_ref,
           attn_ref, og_ref, l_s, rx_attn, rx_og, tbuf, attn_t, wg, g, r1a, r1b, r2, t2, pz, rz, sqs,
           x_s, x_r, z_s, z_r, p_s, p_r, d_s, d_r, c_s, c_r,
           s1_s, s1_r, s2_s, s2_r, rz_s, rz_r, q_s, q_r):
    ns = 4
    nz = nb // 2
    tok, din = attn_ref.shape
    dout = og_ref.shape[1]
    r = w_ref.shape[0]
    half = dout // 2
    block = nb * r
    seq = lax.axis_index("seq")
    batch = lax.axis_index("batch")
    z = batch // 2
    core = batch % 2
    hi = seq // 2
    lo = seq % 2
    sh = (1 - hi) * 2 + lo
    sl = hi * 2 + (1 - lo)
    sd = (1 - hi) * 2 + (1 - lo)
    hi_dev = (sh, batch)
    lo_dev = (sl, batch)
    core_dev = (seq, z * 2 + 1 - core)
    cols_a = pl.ds(0, half)
    cols_b = pl.ds(half, half)

    def other(i):
        f = lax.rem(seq * nb + batch + i, ns * nb)
        return (f // nb, lax.rem(f, nb))

    la = pltpu.make_async_copy(attn_hbm, attn_ref, l_s.at[0])
    la.start()
    lg = pltpu.make_async_copy(og_hbm, og_ref, l_s.at[1])
    lg.start()
    barrier = pltpu.get_barrier_semaphore()

    def greet(i, carry):
        pl.semaphore_signal(barrier, inc=1, device_id=other(i), device_id_type=MESH)
        return carry

    lax.fori_loop(1, ns * nb, greet, 0)
    pl.semaphore_wait(barrier, ns * nb - 1)

    pending = []

    def remote(src, dst, ssem, rsem, dev):
        c = pltpu.make_async_remote_copy(
            src_ref=src, dst_ref=dst, send_sem=ssem, recv_sem=rsem,
            device_id=dev, device_id_type=MESH)
        c.start()
        pending.append(c)
        return c

    near = jnp.minimum(z, nz - 1 - z)

    def zk(t):
        if t == 0:
            return z
        both = t <= 2 * near
        dist = jnp.where(both, (t + 1) // 2, t - near)
        above = jnp.where(both, t % 2, jnp.where(z < nz - 1 - z, 1, 0))
        return z + dist * (2 * above - 1)

    def z_copy(t, up):
        src = zk(t)
        to = jnp.minimum(z + 1, nz - 1) if up else jnp.maximum(z - 1, 0)
        return pltpu.make_async_remote_copy(
            src_ref=shard(t), dst_ref=wg.at[wrows(seq, src)],
            send_sem=z_s.at[nz * up + src], recv_sem=z_r.at[src],
            device_id=(seq, to * 2 + core), device_id_type=MESH)

    def z_pass(t, up):
        src = zk(t)
        if up:
            return jnp.logical_and(src <= z, z < nz - 1)
        return jnp.logical_and(src >= z, z > 0)

    def z_each(t, act):
        for up in (0, 1):
            @pl.when(z_pass(t, up))
            def _():
                act(z_copy(t, up))

    def wrows(s, zz):
        return pl.ds(pl.multiple_of((s * nb + zz * 2 + core) * r, 16), r)

    def shard(k):
        return w_ref if k == 0 else wg.at[wrows(seq, zk(k))]

    own = wrows(seq, z)
    hc, lc, dac, dbc, cc = {}, {}, {}, {}, {}

    def plane_send(k):
        rows = wrows(seq, zk(k))
        hc[k] = remote(shard(k), wg.at[rows], p_s.at[2 * k], p_r.at[2 * k], hi_dev)
        lc[k] = remote(shard(k), wg.at[rows], p_s.at[2 * k + 1], p_r.at[2 * k + 1], lo_dev)

    def core_send(k, j, s):
        rows = wrows(s, zk(k))
        src = w_ref if (k == 0 and j == 0) else wg.at[rows]
        i = 4 * k + j
        cc[i] = remote(src, wg.at[rows], c_s.at[i], c_r.at[i], core_dev)

    def z_arrive(k):
        z_copy(k, 0).wait_recv()
        z_each(k, lambda c: c.start())
        plane_send(k)
        core_send(k, 0, seq)

    def plane_arrive(k):
        hc[k].wait_recv()
        v = wg.at[wrows(sh, zk(k)), cols_a]
        dac[k] = remote(v, v, d_s.at[2 * k], d_r.at[2 * k], lo_dev)
        lc[k].wait_recv()
        v = wg.at[wrows(sl, zk(k)), cols_b]
        dbc[k] = remote(v, v, d_s.at[2 * k + 1], d_r.at[2 * k + 1], hi_dev)
        core_send(k, 1, sh)
        core_send(k, 2, sl)

    def diag_arrive(k):
        dac[k].wait_recv()
        dbc[k].wait_recv()
        core_send(k, 3, sd)

    xa = remote(attn_hbm, rx_attn, x_s.at[0], x_r.at[0], core_dev)
    plane_send(0)
    z_each(0, lambda c: c.start())
    xo = remote(og_hbm, rx_og, x_s.at[1], x_r.at[1], core_dev)
    core_send(0, 0, seq)
    wg[own, :] = w_ref[...]

    def transpose_in(src, koff):
        for s in range(ns):
            tbuf[...] = src[:, s * block:(s + 1) * block].T
            for zz in range(nz):
                part = tbuf[pl.ds(pl.multiple_of((zz * 2 + core) * r, 16), r), :]
                attn_t[pl.ds((s * nz + zz) * r, r), pl.ds(koff, tok)] = part

    tile = 256 if dout % 256 == 0 and din % 256 == 0 else 128
    ntile = dout // tile

    def grad_tiles(first, last):
        def body(i, carry):
            c = pl.ds(pl.multiple_of(i * tile, tile), tile)
            acc = jnp.dot(attn_t[:, :tok], og_ref[:, c], preferred_element_type=F32)
            acc += jnp.dot(attn_t[:, tok:], rx_og[:, c], preferred_element_type=F32)
            g[:, c] = acc.astype(BF16)
            return carry
        lax.fori_loop(first, last, body, 0)

    la.wait()
    transpose_in(attn_ref, 0)
    if nz > 1:
        z_arrive(1)
    xa.wait_recv()
    transpose_in(rx_attn, tok)
    plane_arrive(0)
    xo.wait_recv()
    lg.wait()
    for k in range(1, nz):
        grad_tiles((k - 1) * ntile // (nz - 1), k * ntile // (nz - 1))
        if k + 1 < nz:
            z_arrive(k + 1)
        if k < nz - 1:
            plane_arrive(k)

    def grows(s, i):
        return pl.ds(pl.multiple_of((s * nz + lax.rem(z + 1 + i, nz)) * r, 16), r)

    def rr(i):
        return pl.ds(i * r, r)

    s1, s2 = {}, {}

    def stage1(i):
        s1[i] = [
            remote(g.at[grows(sd, i), cols_a], r1a.at[rr(2 * i + 1)], s1_s.at[4 * i], s1_r.at[4 * i], hi_dev),
            remote(g.at[grows(sd, i), cols_b], r1b.at[rr(2 * i + 1)], s1_s.at[4 * i + 1], s1_r.at[4 * i + 1], lo_dev),
            remote(g.at[grows(sh, i), cols_a], r1a.at[rr(2 * i)], s1_s.at[4 * i + 2], s1_r.at[4 * i + 2], hi_dev),
            remote(g.at[grows(sl, i), cols_b], r1b.at[rr(2 * i)], s1_s.at[4 * i + 3], s1_r.at[4 * i + 3], lo_dev),
        ]

    def stage2(i):
        s1[i][0].wait_recv()
        t2[rr(i), cols_a] = (g[grows(sl, i), cols_a].astype(F32) + r1a[rr(2 * i + 1), :].astype(F32)).astype(BF16)
        ca = remote(t2.at[rr(i), cols_a], r2.at[rr(i), cols_a], s2_s.at[2 * i], s2_r.at[2 * i], lo_dev)
        s1[i][1].wait_recv()
        t2[rr(i), cols_b] = (g[grows(sh, i), cols_b].astype(F32) + r1b[rr(2 * i + 1), :].astype(F32)).astype(BF16)
        cb = remote(t2.at[rr(i), cols_b], r2.at[rr(i), cols_b], s2_s.at[2 * i + 1], s2_r.at[2 * i + 1], hi_dev)
        s2[i] = [ca, cb]

    zsum = {}

    def stage3(i):
        for c in (s1[i][2], s1[i][3], s2[i][0], s2[i][1]):
            c.wait_recv()
        for cols, r1 in ((cols_a, r1a), (cols_b, r1b)):
            v = g[grows(seq, i), cols].astype(F32) + r1[rr(2 * i), :].astype(F32) + r2[rr(i), cols].astype(F32)
            if i == nz - 1:
                gw_ref[:, cols] = v
            else:
                pz[rr(i), cols] = v.astype(BF16)
        if i < nz - 1:
            dev = (seq, lax.rem(z + 1 + i, nz) * 2 + core)
            zsum[i] = remote(pz.at[rr(i)], rz.at[rr(i)], rz_s.at[i], rz_r.at[i], dev)

    stage1(0)
    if nz > 1:
        plane_arrive(nz - 1)
    for k in range(nz):
        diag_arrive(k)
        if k == 0 and nz > 1:
            stage1(1)

    def input_tiles(first, last):
        def body(i, carry):
            c = pl.ds(pl.multiple_of(i * tile, tile), tile)
            v = lax.dot_general(og_ref[...], wg[c, :], (((1,), (1,)), ((), ())), preferred_element_type=F32)
            ig_ref[:, c] = v.astype(BF16)
            return carry
        lax.fori_loop(first, last, body, 0)

    itile = din // tile
    stage2(0)
    for i in range(4 * nz):
        cc[i].wait_recv()
    for i in range(nz):
        input_tiles(i * itile // nz, (i + 1) * itile // nz)
        if i + 2 < nz:
            stage1(i + 2)
        if i + 1 < nz:
            stage2(i + 1)
        stage3(i)
    for i in range(nz - 1):
        zsum[i].wait_recv()
        gw_ref[...] += rz[rr(i), :].astype(F32)

    v = gw_ref[...]
    part = jnp.sum((v * v).reshape(r // 8, 8, dout), axis=0)
    acc = part[:, :128]
    for i in range(1, dout // 128):
        acc += part[:, i * 128:(i + 1) * 128]
    sqs[0] = acc

    def q_copy(i):
        return pltpu.make_async_remote_copy(
            src_ref=sqs.at[0], dst_ref=sqs.at[i], send_sem=q_s.at[i], recv_sem=q_r.at[i],
            device_id=other(i), device_id_type=MESH)

    def q_start(i, carry):
        q_copy(i).start()
        return carry

    def q_wait(i, carry):
        q_copy(i).wait()
        return carry

    lax.fori_loop(1, ns * nb, q_start, 0)
    lax.fori_loop(1, ns * nb, q_wait, 0)
    total = sqs[0]
    for i in range(1, ns * nb):
        total += sqs[i]
    sq_ref[...] = total
    for c in pending:
        c.wait_send()
    for t in range(nz):
        z_each(t, lambda c: c.wait_send())


def fused(attn_out, out_grad, shard_weight, ns, nb):
    tok, din = attn_out.shape
    dout = out_grad.shape[1]
    r = shard_weight.shape[0]
    nz = nb // 2
    n = ns * nb
    dma = lambda k: pltpu.SemaphoreType.DMA((k,))
    vm = pl.BlockSpec(memory_space=pltpu.VMEM)
    pairs = [2, 2 * nz, 2 * nz, 2 * nz, 4 * nz, 4 * nz, 2 * nz, nz, n]
    return pl.pallas_call(
        functools.partial(kernel, nb),
        out_shape=(
            jax.ShapeDtypeStruct((tok, din), BF16),
            jax.ShapeDtypeStruct((r, dout), F32),
            jax.ShapeDtypeStruct((8, 128), F32),
        ),
        in_specs=[pl.BlockSpec(memory_space=pl.ANY)] * 2 + [vm],
        out_specs=(vm,) * 3,
        scratch_shapes=[
            pltpu.VMEM((tok, din), BF16),
            pltpu.VMEM((tok, dout), BF16),
            dma(2),
            pltpu.VMEM((tok, din), BF16),
            pltpu.VMEM((tok, dout), BF16),
            pltpu.VMEM((nb * r, tok), BF16),
            pltpu.VMEM((din // 2, 2 * tok), BF16),
            pltpu.VMEM((din, dout), BF16),
            pltpu.VMEM((din // 2, dout), BF16),
            pltpu.VMEM((2 * nz * r, dout // 2), BF16),
            pltpu.VMEM((2 * nz * r, dout // 2), BF16),
            pltpu.VMEM((nz * r, dout), BF16),
            pltpu.VMEM((nz * r, dout), BF16),
            pltpu.VMEM((nz * r, dout), BF16),
            pltpu.VMEM((nz * r, dout), BF16),
            pltpu.VMEM((n, 8, 128), F32),
        ] + [dma(k) for k in pairs for _ in range(2)],
        compiler_params=pltpu.CompilerParams(
            collective_id=0, has_side_effects=True, vmem_limit_bytes=66_000_000),
    )(attn_out, out_grad, shard_weight)


def plain(attn_out, out_grad, shard_weight):
    projected = lax.dot_general(
        out_grad,
        lax.all_gather(shard_weight, ("seq", "batch"), axis=0, tiled=True),
        (((1,), (1,)), ((), ())),
        preferred_element_type=F32,
    )
    width = out_grad.shape[1] // GRAD_BLOCKS
    parts = []
    for b in range(GRAD_BLOCKS):
        d = lax.dot_general(
            attn_out, out_grad[:, b * width:(b + 1) * width],
            (((0,), (0,)), ((), ())), preferred_element_type=F32).astype(BF16)
        d = lax.psum_scatter(d, "seq", scatter_dimension=0, tiled=True)
        parts.append(lax.psum_scatter(d, "batch", scatter_dimension=0, tiled=True).astype(F32))
    weight_grad = jnp.concatenate(parts, axis=1)
    squares = lax.psum(jnp.sum(weight_grad * weight_grad), ("seq", "batch"))
    return projected.astype(BF16), weight_grad, squares


def on_device(ns, nb, attn_out, out_grad, master, moment_one, moment_two):
    shard_weight = master.astype(BF16)
    r, dout = master.shape
    din = attn_out.shape[1]
    if ns == 4 and nb % 2 == 0 and r % 16 == 0 and (nb * r) % 128 == 0 and dout % 256 == 0:
        input_grad, weight_grad, sq = fused(attn_out, out_grad, shard_weight, ns, nb)
        squares = jnp.sum(sq)
    else:
        input_grad, weight_grad, squares = plain(attn_out, out_grad, shard_weight)
    grad_norm = jnp.sqrt(squares) + 1e-06
    limit = jnp.sqrt(jnp.float32(din * dout))
    clipped = weight_grad * jnp.minimum(jnp.float32(1.0), limit / grad_norm)
    new_one = 0.9 * moment_one + 0.1 * clipped
    new_two = 0.999 * moment_two + 0.001 * clipped * clipped
    first_hat = new_one / (1.0 - 0.9**STEP)
    second_hat = new_two / (1.0 - 0.999**STEP)
    new_master = master - 0.01 * (first_hat / (jnp.sqrt(second_hat) + 1e-08) + 0.1 * master)
    return (input_grad, new_master, new_one, new_two)


def solution(mesh):
    spec = P(("seq", "batch"), None)
    return jax.shard_map(
        functools.partial(on_device, mesh.shape["seq"], mesh.shape["batch"]),
        mesh=mesh,
        in_specs=(spec,) * 5,
        out_specs=(spec,) * 4,
        check_vma=False,
    )
```
